32 devices in a mesh: tm: 4 (over y, x), space: 8 (over z, core).
Axes of the slice: x: 2, y: 2, z: 4, core: 2. Of those that a mesh axis runs over, the one named last changes fastest.
Arguments:
- residual_field: float32 [64, 128, 128, 128], P('tm', 'space'), may hold values from -6 to 6
- eigvec_x: float32 [128, 128], replicated, may hold values from -1 to 1, as said below
- eigvec_y: float32 [128, 128], replicated, may hold values from -1 to 1, as said below
- eigvec_z: float32 [128, 128], replicated, may hold values from -1 to 1, as said below
- eigval_x: float32 [128], replicated, may hold values from 0.0001 to 0.05
- eigval_y: float32 [128], replicated, may hold values from 0.0001 to 0.05
- eigval_z: float32 [128], replicated, may hold values from 0.0001 to 0.05
Outputs:
- update: float32 [64, 128, 128, 128], P('tm', 'space')
The draws below stay inside these ranges and needn't reach their ends.
Inputs may be any that keep to these rules, and one draw needn't show every extreme that they name: `eigvec_x`: an orthogonal matrix. `eigvec_y`: an orthogonal matrix. `eigvec_z`: an orthogonal matrix.
All inputs are finite; a program needn't handle non-finite values.
Results may differ from the reference program's by a relative error of at most 0.00025.
Values sent between devices are 32-bit elements; how exact they have to be, the bound alone decides.
A program may use at most 256 MiB of HBM per device.

```python
import math
import jax
import jax.numpy as jnp
from jax import lax

L = 64
NX = 128
NY = 128
NZ = 128


def orthogonal(key, dimension):

    def reflect(source, matrix):
        vector = jax.random.normal(jax.random.fold_in(key, source), (dimension,), jnp.float32)
        vector = vector / jnp.sqrt(jnp.sum(vector * vector))
        return matrix - 2.0 * jnp.outer(jnp.dot(matrix, vector), vector)
    return lax.fori_loop(0, dimension, reflect, jnp.eye(dimension, dtype=jnp.float32))


def draw_eigvec_x(key, part):
    return orthogonal(jax.random.fold_in(key, 101), NX)


def draw_eigvec_y(key, part):
    return orthogonal(jax.random.fold_in(key, 202), NY)


def draw_eigvec_z(key, part):
    return orthogonal(jax.random.fold_in(key, 303), NZ)


def shard_levels(own_key, dims, cuts, low, top_value):
    gain, own = 1.0, jax.random.fold_in(own_key, 6)
    for position, parts in cuts:
        steps = jnp.exp(jax.random.uniform(jax.random.fold_in(own, position), (parts,), jnp.float32, low / len(cuts), top_value / len(cuts)))
        gain = gain * jnp.repeat(steps, dims[position] // parts).reshape([-1 if axis == position else 1 for axis in range(len(dims))])
    return gain


def gaussian(key, shape, spread, most, pieces=(), held_as=jnp.bfloat16):
    loudness = shard_levels(key, shape, pieces, -0.22, 0.18) if pieces else 1.0
    values = jax.random.normal(key, shape, jnp.float32) * spread * loudness
    return jnp.minimum(jnp.maximum(values, -most), most).astype(held_as)


def setup_inputs(seed: int = 0) -> dict:
    arg_keys = jax.random.split(jax.random.key(seed), 8)
    return {
        "residual_field": gaussian(arg_keys[0], (L, NX, NY, NZ), 1.0, 6.0, ((0, 4), (1, 8)), jnp.float32),
        "eigvec_x": draw_eigvec_x(jax.random.fold_in(arg_keys[7], 71), 0),
        "eigvec_y": draw_eigvec_y(jax.random.fold_in(arg_keys[7], 71), 0),
        "eigvec_z": draw_eigvec_z(jax.random.fold_in(arg_keys[7], 71), 0),
        "eigval_x": jnp.clip(jnp.exp(jax.random.uniform(arg_keys[4], (NX,), jnp.float32, math.log(0.0001), math.log(0.05))), 0.0001, 0.05),
        "eigval_y": jnp.clip(jnp.exp(jax.random.uniform(arg_keys[5], (NY,), jnp.float32, math.log(0.0001), math.log(0.05))), 0.0001, 0.05),
        "eigval_z": jnp.clip(jnp.exp(jax.random.uniform(arg_keys[6], (NZ,), jnp.float32, math.log(0.0001), math.log(0.05))), 0.0001, 0.05),
    }


highest = lax.Precision.HIGHEST
circulant_alpha = 0.01


def spectral_solve(values, shifts, total_steps):
    step_ids = jnp.arange(total_steps, dtype=jnp.int32)
    phases = (step_ids[:, None] * step_ids[None, :]) % total_steps
    angles = (2.0 * math.pi / total_steps) * phases.astype(jnp.float32)
    cosine = jnp.cos(angles)
    sine_table = jnp.sin(angles)
    root_alpha = circulant_alpha ** (1.0 / total_steps)
    powers = root_alpha ** step_ids.astype(jnp.float32)
    flattened = values.reshape(total_steps, -1) * powers[:, None]
    real_part = jnp.dot(cosine, flattened, precision=highest)
    imag_part = -jnp.dot(sine_table, flattened, precision=highest)
    flat_shift = shifts.reshape(1, -1)
    denom_real = 1.0 + flat_shift - root_alpha * cosine[:, 1:2]
    denom_imag = root_alpha * sine_table[:, 1:2]
    modulus = denom_real * denom_real + denom_imag * denom_imag
    quot_real = (real_part * denom_real + imag_part * denom_imag) / modulus
    quot_imag = (imag_part * denom_real - real_part * denom_imag) / modulus
    restored = jnp.dot(cosine, quot_real, precision=highest) - jnp.dot(sine_table, quot_imag, precision=highest)
    restored = restored / (total_steps * powers[:, None])
    return restored.reshape(values.shape)


def reference(residual_field, eigvec_x, eigvec_y, eigvec_z, eigval_x, eigval_y, eigval_z):
    total_steps = residual_field.shape[0]

    def forward_plane(plane):
        plane = jnp.einsum('xyz,zk->xyk', plane, eigvec_z, precision=highest)
        plane = jnp.einsum('xyk,yj->xjk', plane, eigvec_y, precision=highest)
        return jnp.einsum('xjk,xi->ijk', plane, eigvec_x, precision=highest)

    def inverse_plane(plane):
        plane = jnp.einsum('ijk,zk->ijz', plane, eigvec_z, precision=highest)
        plane = jnp.einsum('ijz,yj->iyz', plane, eigvec_y, precision=highest)
        return jnp.einsum('iyz,xi->xyz', plane, eigvec_x, precision=highest)

    coeffs = lax.map(forward_plane, residual_field)
    shift_yz = eigval_y[:, None] + eigval_z[None, :]

    def solve_slab(source):
        slab = lax.dynamic_index_in_dim(coeffs, source, 1, keepdims=False)
        shift_x = lax.dynamic_index_in_dim(eigval_x, source, 0, keepdims=False)
        return spectral_solve(slab, shift_x + shift_yz, total_steps)

    solved = lax.map(solve_slab, jnp.arange(eigval_x.shape[0], dtype=jnp.int32))
    solved = jnp.moveaxis(solved, 0, 1)
    return lax.map(inverse_plane, solved)
```

```python
import functools
import jax
import jax.numpy as jnp
from jax import lax
from jax.experimental import pallas as pl
from jax.experimental.pallas import tpu as pltpu
from jax.sharding import PartitionSpec as P

highest = lax.Precision.HIGHEST
circulant_alpha = 0.01
tile_rows = 8


def halves(a):
    high = a.astype(jnp.bfloat16)
    return high, (a - high.astype(jnp.float32)).astype(jnp.bfloat16)


def stacked(matrix):
    return jnp.concatenate(halves(matrix), axis=0)


def left_product(left, a):
    rows, columns = left.shape[0] // 2, a.shape[1]
    r = jnp.dot(left, jnp.concatenate(halves(a), axis=1), preferred_element_type=jnp.float32)
    return (r[:rows, :columns] + r[rows:, :columns]) + (r[:rows, columns:] + r[rows:, columns:])


def right_product(a, right):
    columns = right.shape[1] // 2
    r = jnp.dot(jnp.concatenate(halves(a), axis=1), right, preferred_element_type=jnp.float32)
    return r[:, :columns] + r[:, columns:]


def power(a, n):
    result = None
    while n:
        if n & 1:
            result = a if result is None else result * a
        a, n = a * a, n >> 1
    return result


def plane_kernel(a_ref, left_ref, right_ref, o_ref):
    left = stacked(left_ref[...])
    right = jnp.concatenate(halves(right_ref[...]), axis=1)
    right = jnp.concatenate([right, right], axis=0)

    def one(x, carry):
        o_ref[0, x] = left_product(left, right_product(a_ref[0, x], right))
        return carry

    lax.fori_loop(0, a_ref.shape[1], one, 0, unroll=4)


def plane_transform(a, left, right):
    steps, rows, size_y, size_z = a.shape
    block = pl.BlockSpec((1, rows, size_y, size_z), lambda t: (t, 0, 0, 0))
    whole = lambda m: pl.BlockSpec(m.shape, lambda t: (0, 0))
    return pl.pallas_call(
        plane_kernel,
        grid=(steps,),
        in_specs=[block, whole(left), whole(right)],
        out_specs=block,
        out_shape=jax.ShapeDtypeStruct(a.shape, jnp.float32),
        compiler_params=pltpu.CompilerParams(vmem_limit_bytes=60 * 2**20),
    )(a, left, right)


def exchange_kernel(
    space_count, time_count, chunks,
    in_ref, vt_ref, v_ref, ex_ref, shift_ref, out_ref,
    recv, fins, own_in, own_out, go_send, go_recv, back_send, back_recv, st_send, st_recv,
):
    steps, rows, band_rows = recv.shape[2], recv.shape[3], recv.shape[4]
    size_z = recv.shape[5]
    band = band_rows * chunks
    me = lax.axis_index("space")
    position = lax.axis_index("tm")

    def peer_of(k):
        return lax.rem(me + k, space_count)

    def timer_of(k):
        return lax.rem(position + k, time_count)

    def columns(owner, c):
        return pl.ds(pl.multiple_of(owner * band + c * band_rows, tile_rows), band_rows)

    def go(c, peer):
        return pltpu.make_async_remote_copy(
            src_ref=in_ref.at[:, :, columns(peer, c), :],
            dst_ref=recv.at[c, me],
            send_sem=go_send.at[c, peer],
            recv_sem=go_recv.at[c, me],
            device_id={"space": peer},
            device_id_type=pl.DeviceIdType.MESH,
        )

    def go_arrival(c, peer):
        return pltpu.make_async_remote_copy(
            src_ref=in_ref.at[:, :, columns(peer, c), :],
            dst_ref=recv.at[c, peer],
            send_sem=go_send.at[c, peer],
            recv_sem=go_recv.at[c, peer],
            device_id={"space": peer},
            device_id_type=pl.DeviceIdType.MESH,
        )

    def back(c, peer):
        return pltpu.make_async_remote_copy(
            src_ref=recv.at[c, peer],
            dst_ref=out_ref.at[:, :, columns(me, c), :],
            send_sem=back_send.at[c, peer],
            recv_sem=back_recv.at[c, me],
            device_id={"space": peer},
            device_id_type=pl.DeviceIdType.MESH,
        )

    def back_arrival(c, peer):
        return pltpu.make_async_remote_copy(
            src_ref=recv.at[c, peer],
            dst_ref=out_ref.at[:, :, columns(peer, c), :],
            send_sem=back_send.at[c, peer],
            recv_sem=back_recv.at[c, peer],
            device_id={"space": peer},
            device_id_type=pl.DeviceIdType.MESH,
        )

    def final(c, peer, owner):
        return pltpu.make_async_remote_copy(
            src_ref=fins.at[c, owner],
            dst_ref=fins.at[c, owner],
            send_sem=st_send.at[c, peer],
            recv_sem=st_recv.at[c, owner],
            device_id={"tm": peer},
            device_id_type=pl.DeviceIdType.MESH,
        )

    def take_own(c):
        return pltpu.make_async_copy(
            in_ref.at[:, :, columns(me, c), :], recv.at[c, me], own_in.at[c]
        )

    def give_own(c):
        return pltpu.make_async_copy(
            recv.at[c, me], out_ref.at[:, :, columns(me, c), :], own_out.at[c]
        )

    barrier = pltpu.get_barrier_semaphore()
    for k in range(1, space_count):
        pl.semaphore_signal(
            barrier, inc=1, device_id={"space": peer_of(k)}, device_id_type=pl.DeviceIdType.MESH
        )
    for k in range(1, time_count):
        pl.semaphore_signal(
            barrier, inc=1, device_id={"tm": timer_of(k)}, device_id_type=pl.DeviceIdType.MESH
        )
    pl.semaphore_wait(barrier, space_count + time_count - 2)

    middle = space_count // 2
    offsets = sorted(range(1, space_count), key=lambda k: abs(k - middle))
    for c in range(chunks):
        for k in offsets:
            go(c, peer_of(k)).start()
        take_own(c).start()

    left = stacked(vt_ref[...])
    left_back = stacked(v_ref[...])
    ex = ex_ref[...]

    def load(c, t, j):
        parts = [
            recv.at[c, s, t].reshape(rows * band_rows, size_z)[pl.ds(j, rows, stride=band_rows), :]
            for s in range(space_count)
        ]
        return jnp.concatenate(parts, axis=0)

    def store(c, t, j, value):
        for s in range(space_count):
            view = recv.at[c, s, t].reshape(rows * band_rows, size_z)
            view[pl.ds(j, rows, stride=band_rows), :] = value[s * rows : (s + 1) * rows]

    def chunk(c, carry):
        for k in offsets:
            go_arrival(c, peer_of(k)).wait_recv()
        take_own(c).wait()
        for j in range(band_rows):
            damping = 1.0 / (1.0 + (ex + shift_ref[c, j : j + 1, :]))

            def forward(t, state, j=j, damping=damping):
                state = damping * (state + left_product(left, load(c, t, j)))
                store(c, t, j, state)
                return state

            fins[c, position, j] = lax.fori_loop(
                0, steps, forward, jnp.zeros_like(damping), unroll=2
            )
        for k in range(1, time_count):
            final(c, timer_of(k), position).start()
        for k in range(1, time_count):
            final(c, timer_of(k), timer_of(k)).wait_recv()
        for j in range(band_rows):
            damping = 1.0 / (1.0 + (ex + shift_ref[c, j : j + 1, :]))
            block_decay = power(damping, steps)
            overall = fins[c, 0, j]
            for p in range(1, time_count):
                overall = block_decay * overall + fins[c, p, j]
            incoming = (circulant_alpha * overall) / (
                1.0 - circulant_alpha * power(block_decay, time_count)
            )
            for p in range(time_count - 1):
                incoming = jnp.where(
                    p < position, block_decay * incoming + fins[c, p, j], incoming
                )

            def inverse(t, incoming, j=j, damping=damping):
                incoming = damping * incoming
                store(c, t, j, left_product(left_back, load(c, t, j) + incoming))
                return incoming

            lax.fori_loop(0, steps, inverse, incoming, unroll=2)
        for k in offsets:
            go(c, peer_of(k)).wait_send()
            back(c, peer_of(k)).start()
        give_own(c).start()
        return carry

    lax.fori_loop(0, chunks, chunk, 0)

    for c in range(chunks):
        for k in range(1, time_count):
            final(c, timer_of(k), position).wait_send()
        for k in offsets:
            back(c, peer_of(k)).wait_send()
            back_arrival(c, peer_of(k)).wait_recv()
        give_own(c).wait()


def exchange_solve(planes, eigvec_x, eigval_x, shift_yz, space_count, time_count):
    steps, rows, size_y, size_z = planes.shape
    band = size_y // space_count
    chunks = 2 if band % (2 * tile_rows) == 0 else 1
    band_rows = band // chunks
    size_x = rows * space_count
    vmem = pl.BlockSpec(memory_space=pltpu.VMEM)
    dma = pltpu.SemaphoreType.DMA
    return pl.pallas_call(
        functools.partial(exchange_kernel, space_count, time_count, chunks),
        in_specs=[pl.BlockSpec(memory_space=pl.ANY)] + [vmem] * 4,
        out_specs=pl.BlockSpec(memory_space=pl.ANY),
        out_shape=jax.ShapeDtypeStruct(planes.shape, jnp.float32),
        scratch_shapes=[
            pltpu.VMEM((chunks, space_count, steps, rows, band_rows, size_z), jnp.float32),
            pltpu.VMEM((chunks, time_count, band_rows, size_x, size_z), jnp.float32),
            dma((chunks,)),
            dma((chunks,)),
            dma((chunks, space_count)),
            dma((chunks, space_count)),
            dma((chunks, space_count)),
            dma((chunks, space_count)),
            dma((chunks, time_count)),
            dma((chunks, time_count)),
        ],
        compiler_params=pltpu.CompilerParams(
            collective_id=0, has_side_effects=True, vmem_limit_bytes=60 * 2**20
        ),
    )(
        planes,
        eigvec_x.T,
        eigvec_x,
        jnp.broadcast_to(eigval_x[:, None], (size_x, size_z)),
        shift_yz.reshape(chunks, band_rows, size_z),
    )


def entering(part, axis, combine, identity):
    place = lax.axis_index(axis)
    gathered = jax.tree.map(lambda a: lax.all_gather(a, axis), part)
    state = jax.tree.map(lambda a, e: jnp.zeros_like(a) + jnp.asarray(e, a.dtype), part, identity)

    def one(step, state):
        return combine(
            state, jax.tree.map(lambda a: lax.dynamic_index_in_dim(a, step, 0, False), gathered)
        )

    return lax.fori_loop(0, place, one, state)


def recurrence_solve(values, shifts, time_count):
    steps_local = values.shape[0]
    damping = 1.0 / (1.0 + shifts)

    def advance(running, step_row):
        running = damping * (running + step_row)
        return (running, running)

    final_state, partial_value = lax.scan(advance, jnp.zeros_like(shifts), values)
    block_decay = damping**steps_local
    position = lax.axis_index("tm")

    def compose(early_map, late_map):
        return (early_map[0] * late_map[0], late_map[0] * early_map[1] + late_map[1])

    lead_power, offset = entering(
        (block_decay, final_state), "tm", compose, (jnp.ones_like(shifts), jnp.zeros_like(shifts))
    )
    tail_power = jnp.power(block_decay, (time_count - 1 - position).astype(jnp.float32))
    overall = lax.psum(tail_power * final_state, "tm")
    start_value = circulant_alpha * overall / (1.0 - circulant_alpha * block_decay**time_count)
    incoming = lead_power * start_value + offset
    exponents = jnp.arange(1, steps_local + 1, dtype=jnp.int32).astype(jnp.float32)
    powers = jnp.power(damping[None], exponents[:, None, None])
    return partial_value + powers * incoming[None]


def narrow_solve(planes, eigvec_x, eigval_x, shift_yz, time_count):
    steps_local, rows_x, size_y, size_z = planes.shape
    planes = planes.reshape(steps_local, rows_x, size_y * size_z)
    x_lines = lax.all_to_all(planes, "space", split_axis=2, concat_axis=1, tiled=True)
    x_lines = jnp.einsum("txm,xi->tim", x_lines, eigvec_x, precision=highest)
    shifts = eigval_x[:, None] + shift_yz.reshape(1, -1)
    x_lines = recurrence_solve(x_lines, shifts, time_count)
    x_lines = jnp.einsum("tim,xi->txm", x_lines, eigvec_x, precision=highest)
    planes = lax.all_to_all(x_lines, "space", split_axis=1, concat_axis=2, tiled=True)
    return planes.reshape(steps_local, rows_x, size_y, size_z)


def shards(residual_field, eigvec_x, eigvec_y, eigvec_z, eigval_x, eigval_y, eigval_z):
    steps_local, rows_x, size_y, size_z = residual_field.shape
    space_count = lax.axis_size("space")
    time_count = lax.axis_size("tm")
    planes = plane_transform(residual_field, eigvec_y.T, eigvec_z)
    band = size_y // space_count
    shift_y = lax.dynamic_slice_in_dim(eigval_y, lax.axis_index("space") * band, band, 0)
    shift_yz = shift_y[:, None] + eigval_z[None, :]
    if band % tile_rows == 0 and rows_x % tile_rows == 0:
        planes = exchange_solve(planes, eigvec_x, eigval_x, shift_yz, space_count, time_count)
    else:
        planes = narrow_solve(planes, eigvec_x, eigval_x, shift_yz, time_count)
    return plane_transform(planes, eigvec_y, eigvec_z.T)


def solution(mesh):
    placed = (P("tm", "space", None, None), P(), P(), P(), P(), P(), P())
    return jax.shard_map(
        shards, mesh=mesh, in_specs=placed, out_specs=P("tm", "space", None, None), check_vma=False
    )
```
